32 devices in a mesh: dp: 4 (over x, y), tp: 8 (over z, core).
Axes of the slice: x: 2, y: 2, z: 4, core: 2. Of those that a mesh axis runs over, the one named last changes fastest.
Arguments:
- x: bfloat16 [512, 8192], P('dp'), parts along dimension 0
- w_gate: bfloat16 [8192, 28672], P(None, 'tp')
- w_up: bfloat16 [8192, 28672], P(None, 'tp')
- w_down: bfloat16 [28672, 8192], P('tp')
Outputs:
- output: bfloat16 [512, 8192], P('dp'), parts along dimension 0
There are 4 independent parts. The reference program is written for one: setup_inputs(seed, part) draws one part's arguments, and reference() takes and returns one part's arrays. A program takes and returns all parts, laid end to end along the dimension named above; an argument that names none is the same for every part.
All inputs are finite; a program needn't handle non-finite values.
Results may differ from the reference program's by a relative error of at most 0.016.
Values are sent between devices in bfloat16 or wider.
A program may use at most 2 GiB of HBM per device.

```python
import jax
import jax.numpy as jnp

ROWS = 128
D = 8192
FF = 28672


def setup_inputs(seed: int = 0, part: int = 0) -> dict:
    kx, kg, ku, kd = jax.random.split(jax.random.key(seed), 4)
    drawn = {
        "x": jax.random.normal(jax.random.fold_in(kx, part), (ROWS, D), jnp.float32),
        "w_gate": jax.random.normal(kg, (D, FF), jnp.float32) * D**-0.5,
        "w_up": jax.random.normal(ku, (D, FF), jnp.float32) * D**-0.5,
        "w_down": jax.random.normal(kd, (FF, D), jnp.float32) * FF**-0.5,
    }
    return {k: v.astype(jnp.bfloat16) for k, v in drawn.items()}


def reference(x, w_gate, w_up, w_down):
    gate = jnp.dot(x, w_gate, preferred_element_type=jnp.float32)
    up = jnp.dot(x, w_up, preferred_element_type=jnp.float32)
    hidden = (jax.nn.silu(gate) * up).astype(jnp.bfloat16)
    return jnp.dot(hidden, w_down, preferred_element_type=jnp.float32).astype(jnp.bfloat16)
```

```python
import functools

import jax
import jax.numpy as jnp
from jax import lax
from jax.experimental import pallas as pl
from jax.experimental.pallas import tpu as pltpu
from jax.sharding import PartitionSpec as P

MESH = pl.DeviceIdType.MESH
FC = 256
A_DEPTH = 3
YC = 512
B_DEPTH = 4
LAG_Z1, LAG_Z2, LAG_Z3, LAG_DONE = 4, 7, 9, 10


def kernel(
    x_hbm, wg_hbm, wu_hbm, wd_hbm, y_hbm,
    x, hidden, wg, wu, wd, own, core_out, core_in, z_out, z_in1, z_in2, y,
    x_sem, wg_sem, wu_sem, wd_sem, y_sem,
    core_ss, core_rs, z1_ss, z1_rs, z2_ss, z2_rs, z3_ss, z3_rs, fin_ss, fin_rs,
):
    rows, depth = x.shape
    half = rows // 2
    na = hidden.shape[0]
    nb = y.shape[0]
    dp = lax.axis_index("dp")
    tp = lax.axis_index("tp")
    chip = tp // 2
    core = tp % 2
    partner = (dp, tp + 1 - 2 * core)
    pair = (dp, tp + 2 - 4 * (chip % 2))
    cross = (dp, 2 * (3 - chip) + core)
    outer = (chip == 0) | (chip == 3)
    inner = jnp.logical_not(outer)
    mine = pl.ds(pl.multiple_of(core * half, half), half)
    theirs = pl.ds(pl.multiple_of((1 - core) * half, half), half)

    def load_a(w_hbm, buf, sem, i):
        slot = lax.rem(i, A_DEPTH)
        cols = pl.ds(pl.multiple_of(i * FC, FC), FC)
        return pltpu.make_async_copy(w_hbm.at[:, cols], buf.at[slot], sem.at[slot])

    def load_b(i):
        slot = lax.rem(i, B_DEPTH)
        cols = pl.ds(pl.multiple_of(i * YC, YC), YC)
        return pltpu.make_async_copy(wd_hbm.at[:, cols], wd.at[slot], wd_sem.at[slot])

    def store_y(c):
        cols = pl.ds(pl.multiple_of(c * YC, YC), YC)
        return pltpu.make_async_copy(y.at[c], y_hbm.at[:, cols], y_sem.at[c])

    def remote(src, dst, ss, rs, c, to):
        return pltpu.make_async_remote_copy(
            src_ref=src, dst_ref=dst, send_sem=ss.at[c], recv_sem=rs.at[c],
            device_id=to, device_id_type=MESH,
        )

    def to_core(c):
        return remote(core_out.at[c], core_in.at[c], core_ss, core_rs, c, partner)

    def to_inner(c):
        return remote(z_out.at[c], z_in1.at[c], z1_ss, z1_rs, c, pair)

    def to_cross(c):
        return remote(z_out.at[c], z_in2.at[c], z2_ss, z2_rs, c, cross)

    def to_outer(c):
        return remote(y.at[c, mine], y.at[c, mine], z3_ss, z3_rs, c, pair)

    def to_partner(c):
        return remote(y.at[c, mine], y.at[c, mine], fin_ss, fin_rs, c, partner)

    def from_partner(c):
        return remote(y.at[c, theirs], y.at[c, theirs], fin_ss, fin_rs, c, partner)

    x_copy = pltpu.make_async_copy(x_hbm, x, x_sem)
    x_copy.start()
    for i in range(A_DEPTH):
        load_a(wg_hbm, wg, wg_sem, i).start()
        load_a(wu_hbm, wu, wu_sem, i).start()

    barrier = pltpu.get_barrier_semaphore()
    pl.semaphore_signal(barrier, inc=1, device_id=partner, device_id_type=MESH)
    pl.semaphore_signal(barrier, inc=1, device_id=pair, device_id_type=MESH)

    @pl.when(inner)
    def _():
        pl.semaphore_signal(barrier, inc=1, device_id=cross, device_id_type=MESH)

    x_copy.wait()

    def step_a(i, _):
        slot = lax.rem(i, A_DEPTH)
        load_a(wg_hbm, wg, wg_sem, i).wait()
        gate = jnp.dot(x[...], wg[slot], preferred_element_type=jnp.float32)
        load_a(wu_hbm, wu, wu_sem, i).wait()
        up = jnp.dot(x[...], wu[slot], preferred_element_type=jnp.float32)
        hidden[i] = (jax.nn.silu(gate) * up).astype(jnp.bfloat16)

        @pl.when(i + A_DEPTH < na)
        def _():
            load_a(wg_hbm, wg, wg_sem, i + A_DEPTH).start()
            load_a(wu_hbm, wu, wu_sem, i + A_DEPTH).start()

        later = i + A_DEPTH - na

        @pl.when((later >= 0) & (later < B_DEPTH))
        def _():
            load_b(later).start()

        return 0

    lax.fori_loop(0, na, step_a, 0)
    for i in range(A_DEPTH, B_DEPTH):
        load_b(i).start()

    @pl.when(outer)
    def _():
        pl.semaphore_wait(barrier, 2)

    @pl.when(inner)
    def _():
        pl.semaphore_wait(barrier, 3)

    def step_b(j, _):
        @pl.when(j < nb)
        def _():
            slot = lax.rem(j, B_DEPTH)
            load_b(j).wait()
            term = jnp.zeros((rows, YC), jnp.float32)
            for k in range(na):
                term += jnp.dot(
                    hidden[k], wd[slot, k * FC:(k + 1) * FC, :],
                    preferred_element_type=jnp.float32,
                )

            @pl.when(core == 0)
            def _():
                own[j] = term[:half]
                core_out[j] = term[half:].astype(jnp.bfloat16)

            @pl.when(core == 1)
            def _():
                own[j] = term[half:]
                core_out[j] = term[:half].astype(jnp.bfloat16)

            to_core(j).start()

            @pl.when(j + B_DEPTH < nb)
            def _():
                load_b(j + B_DEPTH).start()

        c1 = j - 1

        @pl.when((c1 >= 0) & (c1 < nb))
        def _():
            to_core(c1).wait_recv()
            total = own[c1] + core_in[c1].astype(jnp.float32)

            @pl.when(outer)
            def _():
                z_out[c1] = total.astype(jnp.bfloat16)
                to_inner(c1).start()

            @pl.when(inner)
            def _():
                own[c1] = total

        c2 = j - LAG_Z1

        @pl.when(inner & (c2 >= 0) & (c2 < nb))
        def _():
            to_inner(c2).wait_recv()
            z_out[c2] = (own[c2] + z_in1[c2].astype(jnp.float32)).astype(jnp.bfloat16)
            to_cross(c2).start()

        c3 = j - LAG_Z2

        @pl.when(inner & (c3 >= 0) & (c3 < nb))
        def _():
            to_cross(c3).wait_recv()
            y[c3, mine] = (
                z_out[c3].astype(jnp.float32) + z_in2[c3].astype(jnp.float32)
            ).astype(jnp.bfloat16)
            to_outer(c3).start()
            to_partner(c3).start()

        c4 = j - LAG_Z3

        @pl.when(outer & (c4 >= 0) & (c4 < nb))
        def _():
            to_outer(c4).wait_recv()
            to_partner(c4).start()

        c5 = j - LAG_DONE

        @pl.when((c5 >= 0) & (c5 < nb))
        def _():
            from_partner(c5).wait_recv()
            store_y(c5).start()

        return 0

    lax.fori_loop(0, nb + LAG_DONE, step_b, 0)

    def drain(c, _):
        store_y(c).wait()
        to_core(c).wait_send()
        to_partner(c).wait_send()

        @pl.when(outer)
        def _():
            to_inner(c).wait_send()

        @pl.when(inner)
        def _():
            to_cross(c).wait_send()
            to_outer(c).wait_send()

        return 0

    lax.fori_loop(0, nb, drain, 0)


def solution(mesh):
    def step(x, w_gate, w_up, w_down):
        rows, depth = x.shape
        ff = w_gate.shape[1]
        half = rows // 2
        na, nb = ff // FC, depth // YC
        bf16, f32 = jnp.bfloat16, jnp.float32
        hbm = pl.BlockSpec(memory_space=pltpu.HBM)
        dma = pltpu.SemaphoreType.DMA
        return pl.pallas_call(
            kernel,
            out_shape=jax.ShapeDtypeStruct((rows, depth), bf16),
            in_specs=[hbm] * 4,
            out_specs=hbm,
            scratch_shapes=[
                pltpu.VMEM((rows, depth), bf16),
                pltpu.VMEM((na, rows, FC), bf16),
                pltpu.VMEM((A_DEPTH, depth, FC), bf16),
                pltpu.VMEM((A_DEPTH, depth, FC), bf16),
                pltpu.VMEM((B_DEPTH, ff, YC), bf16),
                pltpu.VMEM((nb, half, YC), f32),
                pltpu.VMEM((nb, half, YC), bf16),
                pltpu.VMEM((nb, half, YC), bf16),
                pltpu.VMEM((nb, half, YC), bf16),
                pltpu.VMEM((nb, half, YC), bf16),
                pltpu.VMEM((nb, half, YC), bf16),
                pltpu.VMEM((nb, rows, YC), bf16),
                dma, dma((A_DEPTH,)), dma((A_DEPTH,)), dma((B_DEPTH,)), dma((nb,)),
            ] + [dma((nb,))] * 10,
            compiler_params=pltpu.CompilerParams(
                collective_id=0, has_side_effects=True, vmem_limit_bytes=64 * 1024 * 1000
            ),
            cost_estimate=pl.CostEstimate(
                flops=6 * rows * depth * ff, bytes_accessed=6 * depth * ff, transcendentals=rows * ff
            ),
        )(x, w_gate, w_up, w_down)

    return jax.shard_map(
        step,
        mesh=mesh,
        in_specs=(P("dp", None), P(None, "tp"), P(None, "tp"), P("tp", None)),
        out_specs=P("dp", None),
        check_vma=False,
    )
```

```python
import functools

import jax
import jax.numpy as jnp
from jax import lax
from jax.experimental import pallas as pl
from jax.experimental.pallas import tpu as pltpu
from jax.sharding import PartitionSpec as P

MESH = pl.DeviceIdType.MESH
FC = 256
YC = 512
NBUF = 8
W = 2
SHARED = 0
FIRST = 5
LAG_NB = 2
PIECES = 8
X0, Z0 = 1, 4
LAG_C, LAG_Z1, LAG_Z2, LAG_Z3 = 1, 4, 7, 9
B_PRIORITY = 0


def kernel(
    x_hbm, wg_hbm, wu_hbm, wd_hbm, y,
    xx, hidden, sent, ring, own, core_out, core_in, z_out, z_in1, z_in2,
    x_sem, ring_sem,
    core_ss, core_rs, z1_ss, z1_rs, z2_ss, z2_rs, z3_ss, z3_rs, fin_ss, fin_rs,
    xa_ss, xa_rs, xz_ss, xz_rs, xc_ss, xc_rs, xd_ss, xd_rs, h_ss, h_rs,
):
    rows, depth = x_hbm.shape
    half = rows // 2
    na = hidden.shape[0]
    nb = depth // YC
    ff = na * FC
    plain = na - 2 * SHARED
    first = min(FIRST, plain)
    loads = plain + SHARED
    quarter = depth // 4
    width = quarter // PIECES

    dp = lax.axis_index("dp")
    tp = lax.axis_index("tp")
    chip = tp // 2
    core = tp % 2
    side = dp // 2
    partner = (dp, tp + 1 - 2 * core)
    pair = (dp, tp + 2 - 4 * (chip % 2))
    cross = (dp, 2 * (3 - chip) + core)
    twin = ((dp + 2) % 4, tp)
    outer = (chip == 0) | (chip == 3)
    inner = jnp.logical_not(outer)
    mine = pl.ds(pl.multiple_of(core * half, half), half)
    theirs = pl.ds(pl.multiple_of((1 - core) * half, half), half)

    def chunk(i):
        shared = plain + 2 * (i - first) + side
        return jnp.where(i < first, i, jnp.where(i < first + SHARED, shared, i - SHARED))

    def load_a(w_hbm, i, which):
        slot = lax.rem(2 * i + which, NBUF)
        cols = pl.ds(pl.multiple_of(chunk(i) * FC, FC), FC)
        return pltpu.make_async_copy(w_hbm.at[:, cols], ring.at[slot], ring_sem.at[slot, 0])

    def load_b(j):
        slot = lax.rem(2 * loads + j, NBUF)
        return [
            pltpu.make_async_copy(
                wd_hbm.at[:, pl.ds(pl.multiple_of(j * YC + p * FC, FC), FC)],
                ring.at[slot, pl.ds(p * ff, ff)],
                ring_sem.at[slot, p],
            )
            for p in range(YC // FC)
        ]

    def start_b(j):
        for copy in load_b(j):
            copy.start(priority=B_PRIORITY)

    def start_item(i, which):
        @pl.when(i < loads)
        def _():
            load_a(wu_hbm if which else wg_hbm, i, which).start()

        @pl.when((i >= loads) & (2 * (i - loads) + which < nb))
        def _():
            start_b(2 * (i - loads) + which)

    def remote(src, dst, ss, rs, c, to):
        return pltpu.make_async_remote_copy(
            src_ref=src, dst_ref=dst, send_sem=ss.at[c], recv_sem=rs.at[c],
            device_id=to, device_id_type=MESH,
        )

    def ycols(c):
        return pl.ds(pl.multiple_of(c * YC, YC), YC)

    def to_core(c):
        return remote(core_out.at[c], core_in.at[c], core_ss, core_rs, c, partner)

    def to_inner(c):
        return remote(z_out.at[c], z_in1.at[c], z1_ss, z1_rs, c, pair)

    def to_cross(c):
        return remote(z_out.at[c], z_in2.at[c], z2_ss, z2_rs, c, cross)

    def to_outer(c):
        part = y.at[mine, ycols(c)]
        return remote(part, part, z3_ss, z3_rs, c, pair)

    def to_partner(c):
        part = y.at[mine, ycols(c)]
        return remote(part, part, fin_ss, fin_rs, c, partner)

    def from_partner(c):
        part = y.at[theirs, ycols(c)]
        return remote(part, part, fin_ss, fin_rs, c, partner)

    def piece(z, c, k):
        return pl.ds(pl.multiple_of((2 * z + c) * quarter + k * width, width), width)

    zpar = chip % 2

    def x_to_twin(k):
        cols = piece(zpar, core, k)
        return remote(xx.at[0, :, cols], xx.at[1, :, cols], xa_ss, xa_rs, k, twin)

    def x_to_pair(k):
        part = xx.at[1, :, piece(zpar, core, k)]
        return remote(part, part, xz_ss, xz_rs, k, pair)

    def x_from_pair(k):
        part = xx.at[1, :, piece(1 - zpar, core, k)]
        return remote(part, part, xz_ss, xz_rs, k, pair)

    def x_to_core(k):
        part = xx.at[1, :, piece(zpar, core, k)]
        return remote(part, part, xc_ss, xc_rs, k, partner)

    def x_from_core(k):
        part = xx.at[1, :, piece(zpar, 1 - core, k)]
        return remote(part, part, xc_ss, xc_rs, k, partner)

    def xz_to_core(k):
        part = xx.at[1, :, piece(1 - zpar, core, k)]
        return remote(part, part, xd_ss, xd_rs, k, partner)

    def xz_from_core(k):
        part = xx.at[1, :, piece(1 - zpar, 1 - core, k)]
        return remote(part, part, xd_ss, xd_rs, k, partner)

    def h_to_twin(t):
        there = hidden.at[plain + 2 * t + side]
        return remote(sent.at[t], there, h_ss, h_rs, t, twin)

    def h_from_twin(t):
        here = hidden.at[plain + 2 * t + 1 - side]
        return remote(sent.at[t], here, h_ss, h_rs, t, twin)

    def forward(s):
        if not SHARED:
            return
        kx = s - X0

        @pl.when((kx >= 0) & (kx < PIECES))
        def _():
            x_to_twin(kx).wait_recv()
            x_to_pair(kx).start()
            x_to_core(kx).start()

        kz = s - Z0

        @pl.when((kz >= 0) & (kz < PIECES))
        def _():
            x_from_pair(kz).wait_recv()
            xz_to_core(kz).start()

    x_copies = [
        pltpu.make_async_copy(
            x_hbm.at[:, pl.ds(q * quarter, quarter)],
            xx.at[0, :, pl.ds(q * quarter, quarter)],
            x_sem.at[q],
        )
        for q in range(4)
    ]
    for copy in x_copies:
        copy.start()
    for i in range(W // 2):
        load_a(wg_hbm, i, 0).start()
        load_a(wu_hbm, i, 1).start()

    barrier = pltpu.get_barrier_semaphore()
    peers = [partner, pair] + ([twin] if SHARED else [])
    for peer in peers:
        pl.semaphore_signal(barrier, inc=1, device_id=peer, device_id_type=MESH)

    @pl.when(inner)
    def _():
        pl.semaphore_signal(barrier, inc=1, device_id=cross, device_id_type=MESH)

    for copy in x_copies:
        copy.wait()

    def meet():
        @pl.when(outer)
        def _():
            pl.semaphore_wait(barrier, len(peers))

        @pl.when(inner)
        def _():
            pl.semaphore_wait(barrier, len(peers) + 1)

    if SHARED:
        meet()
    if SHARED:
        for k in range(PIECES):
            x_to_twin(k).start()

    def gated(gate, up):
        return (jax.nn.silu(gate) * up).astype(jnp.bfloat16)

    def step_a(i, _):
        if SHARED:
            n = i - LAG_NB
            t = n - first

            @pl.when(t == 0)
            def _():
                def arrive(k, _):
                    x_from_core(k).wait_recv()
                    xz_from_core(k).wait_recv()
                    return 0

                lax.fori_loop(0, PIECES, arrive, 0)

            @pl.when((t >= 0) & (t < SHARED))
            def _():
                slot = lax.rem(2 * n, NBUF)
                gate = jnp.dot(xx[1], ring[slot], preferred_element_type=jnp.float32)
                up = jnp.dot(xx[1], ring[slot + 1], preferred_element_type=jnp.float32)
                sent[t] = gated(gate, up)
                h_to_twin(t).start()

        @pl.when(i < loads)
        def _():
            slot = lax.rem(2 * i, NBUF)
            forward(2 * i)
            load_a(wg_hbm, i, 0).wait()
            start_item(i + W // 2, 0)
            gate = jnp.dot(xx[0], ring[slot], preferred_element_type=jnp.float32)
            forward(2 * i + 1)
            load_a(wu_hbm, i, 1).wait()
            start_item(i + W // 2, 1)
            up = jnp.dot(xx[0], ring[slot + 1], preferred_element_type=jnp.float32)
            hidden[chunk(i)] = gated(gate, up)

        return 0

    extra = max(0, first + SHARED + LAG_NB - loads) if SHARED else 0
    lax.fori_loop(0, loads + extra, step_a, 0)
    if not SHARED:
        meet()
    for t in range(SHARED):
        h_from_twin(t).wait_recv()

    def step_b(j, _):
        @pl.when(j < nb)
        def _():
            slot = lax.rem(2 * loads + j, NBUF)
            for copy in load_b(j):
                copy.wait()

            @pl.when(j + W < nb)
            def _():
                start_b(j + W)

            terms = [jnp.zeros((rows, FC), jnp.float32) for _ in range(YC // FC)]
            for k in range(na):
                for p in range(YC // FC):
                    at = p * ff + k * FC
                    terms[p] += jnp.dot(
                        hidden[k], ring[slot, at:at + FC, :],
                        preferred_element_type=jnp.float32,
                    )
            for p, term in enumerate(terms):
                cols = pl.ds(p * FC, FC)

                @pl.when(core == 0)
                def _():
                    own[j, :, cols] = term[:half]
                    core_out[j, :, cols] = term[half:].astype(jnp.bfloat16)

                @pl.when(core == 1)
                def _():
                    own[j, :, cols] = term[half:]
                    core_out[j, :, cols] = term[:half].astype(jnp.bfloat16)

            to_core(j).start()

        c1 = j - LAG_C

        @pl.when((c1 >= 0) & (c1 < nb))
        def _():
            to_core(c1).wait_recv()
            total = own[c1] + core_in[c1].astype(jnp.float32)

            @pl.when(outer)
            def _():
                z_out[c1] = total.astype(jnp.bfloat16)
                to_inner(c1).start()

            @pl.when(inner)
            def _():
                own[c1] = total

        c2 = j - LAG_Z1

        @pl.when(inner & (c2 >= 0) & (c2 < nb))
        def _():
            to_inner(c2).wait_recv()
            z_out[c2] = (own[c2] + z_in1[c2].astype(jnp.float32)).astype(jnp.bfloat16)
            to_cross(c2).start()

        c3 = j - LAG_Z2

        @pl.when(inner & (c3 >= 0) & (c3 < nb))
        def _():
            to_cross(c3).wait_recv()
            y[mine, ycols(c3)] = (
                z_out[c3].astype(jnp.float32) + z_in2[c3].astype(jnp.float32)
            ).astype(jnp.bfloat16)
            to_outer(c3).start()
            to_partner(c3).start()

        c4 = j - LAG_Z3

        @pl.when(outer & (c4 >= 0) & (c4 < nb))
        def _():
            to_outer(c4).wait_recv()
            to_partner(c4).start()

        return 0

    lax.fori_loop(0, nb + LAG_Z3, step_b, 0)

    def drain(c, _):
        to_core(c).wait_send()
        to_partner(c).wait_send()
        from_partner(c).wait_recv()

        @pl.when(outer)
        def _():
            to_inner(c).wait_send()

        @pl.when(inner)
        def _():
            to_cross(c).wait_send()
            to_outer(c).wait_send()

        return 0

    lax.fori_loop(0, nb, drain, 0)
    if SHARED:
        def drain_x(k, _):
            x_to_twin(k).wait_send()
            x_to_pair(k).wait_send()
            x_to_core(k).wait_send()
            xz_to_core(k).wait_send()
            return 0

        lax.fori_loop(0, PIECES, drain_x, 0)
        for t in range(SHARED):
            h_to_twin(t).wait_send()


def solution(mesh):
    def step(x, w_gate, w_up, w_down):
        rows, depth = x.shape
        ff = w_gate.shape[1]
        half = rows // 2
        na, nb = ff // FC, depth // YC
        bf16, f32 = jnp.bfloat16, jnp.float32
        hbm = pl.BlockSpec(memory_space=pltpu.HBM)
        dma = pltpu.SemaphoreType.DMA
        slots = max(SHARED, 1)
        return pl.pallas_call(
            kernel,
            out_shape=jax.ShapeDtypeStruct((rows, depth), bf16),
            in_specs=[hbm] * 4,
            out_specs=pl.BlockSpec(memory_space=pltpu.VMEM),
            scratch_shapes=[
                pltpu.VMEM((2, rows, depth), bf16),
                pltpu.VMEM((na, rows, FC), bf16),
                pltpu.VMEM((slots, rows, FC), bf16),
                pltpu.VMEM((NBUF, depth, FC), bf16),
                pltpu.VMEM((nb, half, YC), f32),
            ] + [pltpu.VMEM((nb, half, YC), bf16)] * 5 + [
                dma((4,)), dma((NBUF, 2)),
            ] + [dma((nb,))] * 10 + [dma((PIECES,))] * 8 + [dma((slots,))] * 2,
            compiler_params=pltpu.CompilerParams(
                collective_id=0, has_side_effects=True, vmem_limit_bytes=50 * 1024 * 1024
            ),
            cost_estimate=pl.CostEstimate(
                flops=6 * rows * depth * ff, bytes_accessed=6 * depth * ff, transcendentals=rows * ff
            ),
        )(pltpu.with_memory_space_constraint(x, pltpu.HBM), w_gate, w_up, w_down)

    return jax.shard_map(
        step,
        mesh=mesh,
        in_specs=(P("dp", None), P(None, "tp"), P(None, "tp"), P("tp", None)),
        out_specs=P("dp", None),
        check_vma=False,
    )
```

```python
import functools

import jax
import jax.numpy as jnp
from jax import lax
from jax.experimental import pallas as pl
from jax.experimental.pallas import tpu as pltpu
from jax.sharding import PartitionSpec as P

MESH = pl.DeviceIdType.MESH
FC = 256
YC = 512
NBUF = 8
W = 4
SHARED = 2
FIRST = 7
LAG_NB = 2
PIECES = 8
X0, Z0 = 6, 9
LAG_C, LAG_Z1, LAG_Z2, LAG_Z3 = 1, 4, 7, 9
B_PRIORITY = 1


def kernel(
    x_hbm, wg_hbm, wu_hbm, wd_hbm, y,
    xx, hidden, sent, ring, own, core_out, core_in, z_out, z_in1, z_in2,
    x_sem, ring_sem,
    core_ss, core_rs, z1_ss, z1_rs, z2_ss, z2_rs, z3_ss, z3_rs, fin_ss, fin_rs,
    xa_ss, xa_rs, xz_ss, xz_rs, xc_ss, xc_rs, xd_ss, xd_rs, h_ss, h_rs,
):
    rows, depth = x_hbm.shape
    half = rows // 2
    na = hidden.shape[0]
    nb = depth // YC
    ff = na * FC
    plain = na - 2 * SHARED
    first = min(FIRST, plain)
    loads = plain + SHARED
    quarter = depth // 4
    width = quarter // PIECES

    dp = lax.axis_index("dp")
    tp = lax.axis_index("tp")
    chip = tp // 2
    core = tp % 2
    side = dp // 2
    partner = (dp, tp + 1 - 2 * core)
    pair = (dp, tp + 2 - 4 * (chip % 2))
    cross = (dp, 2 * (3 - chip) + core)
    twin = ((dp + 2) % 4, tp)
    outer = (chip == 0) | (chip == 3)
    inner = jnp.logical_not(outer)
    mine = pl.ds(pl.multiple_of(core * half, half), half)
    theirs = pl.ds(pl.multiple_of((1 - core) * half, half), half)

    def chunk(i):
        shared = plain + 2 * (i - first) + side
        return jnp.where(i < first, i, jnp.where(i < first + SHARED, shared, i - SHARED))

    def load_a(w_hbm, i, which):
        slot = lax.rem(2 * i + which, NBUF)
        cols = pl.ds(pl.multiple_of(chunk(i) * FC, FC), FC)
        return pltpu.make_async_copy(w_hbm.at[:, cols], ring.at[slot], ring_sem.at[slot, 0])

    def load_b(j):
        slot = lax.rem(2 * loads + j, NBUF)
        return [
            pltpu.make_async_copy(
                wd_hbm.at[:, pl.ds(pl.multiple_of(j * YC + p * FC, FC), FC)],
                ring.at[slot, pl.ds(p * ff, ff)],
                ring_sem.at[slot, p],
            )
            for p in range(YC // FC)
        ]

    def start_b(j):
        for copy in load_b(j):
            copy.start(priority=B_PRIORITY)

    def start_item(i, which):
        @pl.when(i < loads)
        def _():
            load_a(wu_hbm if which else wg_hbm, i, which).start(priority=1)

        @pl.when((i >= loads) & (2 * (i - loads) + which < nb))
        def _():
            start_b(2 * (i - loads) + which)

    def remote(src, dst, ss, rs, c, to):
        return pltpu.make_async_remote_copy(
            src_ref=src, dst_ref=dst, send_sem=ss.at[c], recv_sem=rs.at[c],
            device_id=to, device_id_type=MESH,
        )

    def ycols(c):
        return pl.ds(pl.multiple_of(c * YC, YC), YC)

    def to_core(c):
        return remote(core_out.at[c], core_in.at[c], core_ss, core_rs, c, partner)

    def to_inner(c):
        return remote(z_out.at[c], z_in1.at[c], z1_ss, z1_rs, c, pair)

    def to_cross(c):
        return remote(z_out.at[c], z_in2.at[c], z2_ss, z2_rs, c, cross)

    def to_outer(c):
        part = y.at[mine, ycols(c)]
        return remote(part, part, z3_ss, z3_rs, c, pair)

    def to_partner(c):
        part = y.at[mine, ycols(c)]
        return remote(part, part, fin_ss, fin_rs, c, partner)

    def from_partner(c):
        part = y.at[theirs, ycols(c)]
        return remote(part, part, fin_ss, fin_rs, c, partner)

    def piece(z, c, k):
        return pl.ds(pl.multiple_of((2 * z + c) * quarter + k * width, width), width)

    zpar = chip % 2

    def x_to_twin(k):
        cols = piece(zpar, core, k)
        return remote(xx.at[0, :, cols], xx.at[1, :, cols], xa_ss, xa_rs, k, twin)

    def x_to_pair(k):
        part = xx.at[1, :, piece(zpar, core, k)]
        return remote(part, part, xz_ss, xz_rs, k, pair)

    def x_from_pair(k):
        part = xx.at[1, :, piece(1 - zpar, core, k)]
        return remote(part, part, xz_ss, xz_rs, k, pair)

    def x_to_core(k):
        part = xx.at[1, :, piece(zpar, core, k)]
        return remote(part, part, xc_ss, xc_rs, k, partner)

    def x_from_core(k):
        part = xx.at[1, :, piece(zpar, 1 - core, k)]
        return remote(part, part, xc_ss, xc_rs, k, partner)

    def xz_to_core(k):
        part = xx.at[1, :, piece(1 - zpar, core, k)]
        return remote(part, part, xd_ss, xd_rs, k, partner)

    def xz_from_core(k):
        part = xx.at[1, :, piece(1 - zpar, 1 - core, k)]
        return remote(part, part, xd_ss, xd_rs, k, partner)

    def h_to_twin(t):
        there = hidden.at[plain + 2 * t + side]
        return remote(sent.at[t], there, h_ss, h_rs, t, twin)

    def h_from_twin(t):
        here = hidden.at[plain + 2 * t + 1 - side]
        return remote(sent.at[t], here, h_ss, h_rs, t, twin)

    def forward(s):
        if not SHARED:
            return
        kx = s - X0

        @pl.when((kx >= 0) & (kx < PIECES))
        def _():
            x_to_twin(kx).wait_recv()
            x_to_pair(kx).start()
            x_to_core(kx).start()

        kz = s - Z0

        @pl.when((kz >= 0) & (kz < PIECES))
        def _():
            x_from_pair(kz).wait_recv()
            xz_to_core(kz).start()

    x_copies = [
        pltpu.make_async_copy(
            x_hbm.at[:, pl.ds(q * quarter, quarter)],
            xx.at[0, :, pl.ds(q * quarter, quarter)],
            x_sem.at[q],
        )
        for q in range(4)
    ]
    for copy in x_copies:
        copy.start()
    for n in range(W):
        load_a(wu_hbm if n % 2 else wg_hbm, n // 2, n % 2).start(priority=1)

    barrier = pltpu.get_barrier_semaphore()
    peers = [partner, pair] + ([twin] if SHARED else [])
    for peer in peers:
        pl.semaphore_signal(barrier, inc=1, device_id=peer, device_id_type=MESH)

    @pl.when(inner)
    def _():
        pl.semaphore_signal(barrier, inc=1, device_id=cross, device_id_type=MESH)

    for copy in x_copies:
        copy.wait()

    def meet():
        @pl.when(outer)
        def _():
            pl.semaphore_wait(barrier, len(peers))

        @pl.when(inner)
        def _():
            pl.semaphore_wait(barrier, len(peers) + 1)

    if SHARED:
        meet()
    if SHARED:
        for k in range(PIECES):
            x_to_twin(k).start()

    def gated(gate, up):
        return (jax.nn.silu(gate) * up).astype(jnp.bfloat16)

    def step_a(i, _):
        if SHARED:
            n = i - LAG_NB
            t = n - first

            @pl.when(t == 0)
            def _():
                def arrive(k, _):
                    x_from_core(k).wait_recv()
                    xz_from_core(k).wait_recv()
                    return 0

                lax.fori_loop(0, PIECES, arrive, 0)

            @pl.when((t >= 0) & (t < SHARED))
            def _():
                slot = lax.rem(2 * n, NBUF)
                gate = jnp.dot(xx[1], ring[slot], preferred_element_type=jnp.float32)
                up = jnp.dot(xx[1], ring[slot + 1], preferred_element_type=jnp.float32)
                sent[t] = gated(gate, up)
                h_to_twin(t).start()

        @pl.when(i < loads)
        def _():
            slot = lax.rem(2 * i, NBUF)
            forward(2 * i)
            load_a(wg_hbm, i, 0).wait()
            start_item(i + W // 2, W % 2)
            gate = jnp.dot(xx[0], ring[slot], preferred_element_type=jnp.float32)
            forward(2 * i + 1)
            load_a(wu_hbm, i, 1).wait()
            start_item(i + (W + 1) // 2, 1 - W % 2)
            up = jnp.dot(xx[0], ring[slot + 1], preferred_element_type=jnp.float32)
            hidden[chunk(i)] = gated(gate, up)

        return 0

    extra = max(0, first + SHARED + LAG_NB - loads) if SHARED else 0
    lax.fori_loop(0, loads + extra, step_a, 0)
    if not SHARED:
        meet()
    for t in range(SHARED):
        h_from_twin(t).wait_recv()

    def step_b(j, _):
        @pl.when(j < nb)
        def _():
            slot = lax.rem(2 * loads + j, NBUF)
            for copy in load_b(j):
                copy.wait()

            @pl.when(j + W < nb)
            def _():
                start_b(j + W)

            terms = [jnp.zeros((rows, FC), jnp.float32) for _ in range(YC // FC)]
            for k in range(na):
                for p in range(YC // FC):
                    at = p * ff + k * FC
                    terms[p] += jnp.dot(
                        hidden[k], ring[slot, at:at + FC, :],
                        preferred_element_type=jnp.float32,
                    )
            for p, term in enumerate(terms):
                cols = pl.ds(p * FC, FC)

                @pl.when(core == 0)
                def _():
                    own[j, :, cols] = term[:half]
                    core_out[j, :, cols] = term[half:].astype(jnp.bfloat16)

                @pl.when(core == 1)
                def _():
                    own[j, :, cols] = term[half:]
                    core_out[j, :, cols] = term[:half].astype(jnp.bfloat16)

            to_core(j).start()

        c1 = j - LAG_C

        @pl.when((c1 >= 0) & (c1 < nb))
        def _():
            to_core(c1).wait_recv()
            total = own[c1] + core_in[c1].astype(jnp.float32)

            @pl.when(outer)
            def _():
                z_out[c1] = total.astype(jnp.bfloat16)
                to_inner(c1).start()

            @pl.when(inner)
            def _():
                own[c1] = total

        c3 = j - LAG_Z2

        @pl.when(inner & (c3 >= 0) & (c3 < nb))
        def _():
            to_cross(c3).wait_recv()
            y[mine, ycols(c3)] = (
                z_out[c3].astype(jnp.float32) + z_in2[c3].astype(jnp.float32)
            ).astype(jnp.bfloat16)
            to_outer(c3).start()
            to_partner(c3).start()

        c2 = j - LAG_Z1

        @pl.when(inner & (c2 >= 0) & (c2 < nb))
        def _():
            to_inner(c2).wait_recv()
            z_out[c2] = (own[c2] + z_in1[c2].astype(jnp.float32)).astype(jnp.bfloat16)
            to_cross(c2).start()

        c4 = j - LAG_Z3

        @pl.when(outer & (c4 >= 0) & (c4 < nb))
        def _():
            to_outer(c4).wait_recv()
            to_partner(c4).start()

        return 0

    lax.fori_loop(0, nb + LAG_Z3, step_b, 0)

    def drain(c, _):
        to_core(c).wait_send()
        to_partner(c).wait_send()
        from_partner(c).wait_recv()

        @pl.when(outer)
        def _():
            to_inner(c).wait_send()

        @pl.when(inner)
        def _():
            to_cross(c).wait_send()
            to_outer(c).wait_send()

        return 0

    lax.fori_loop(0, nb, drain, 0)
    if SHARED:
        def drain_x(k, _):
            x_to_twin(k).wait_send()
            x_to_pair(k).wait_send()
            x_to_core(k).wait_send()
            xz_to_core(k).wait_send()
            return 0

        lax.fori_loop(0, PIECES, drain_x, 0)
        for t in range(SHARED):
            h_to_twin(t).wait_send()


def solution(mesh):
    def step(x, w_gate, w_up, w_down):
        rows, depth = x.shape
        ff = w_gate.shape[1]
        half = rows // 2
        na, nb = ff // FC, depth // YC
        bf16, f32 = jnp.bfloat16, jnp.float32
        hbm = pl.BlockSpec(memory_space=pltpu.HBM)
        dma = pltpu.SemaphoreType.DMA
        slots = max(SHARED, 1)
        return pl.pallas_call(
            kernel,
            out_shape=jax.ShapeDtypeStruct((rows, depth), bf16),
            in_specs=[hbm] * 4,
            out_specs=pl.BlockSpec(memory_space=pltpu.VMEM),
            scratch_shapes=[
                pltpu.VMEM((2, rows, depth), bf16),
                pltpu.VMEM((na, rows, FC), bf16),
                pltpu.VMEM((slots, rows, FC), bf16),
                pltpu.VMEM((NBUF, depth, FC), bf16),
                pltpu.VMEM((nb, half, YC), f32),
            ] + [pltpu.VMEM((nb, half, YC), bf16)] * 5 + [
                dma((4,)), dma((NBUF, 2)),
            ] + [dma((nb,))] * 10 + [dma((PIECES,))] * 8 + [dma((slots,))] * 2,
            compiler_params=pltpu.CompilerParams(
                collective_id=0, has_side_effects=True, vmem_limit_bytes=50 * 1024 * 1024
            ),
            cost_estimate=pl.CostEstimate(
                flops=6 * rows * depth * ff, bytes_accessed=6 * depth * ff, transcendentals=rows * ff
            ),
        )(pltpu.with_memory_space_constraint(x, pltpu.HBM), w_gate, w_up, w_down)

    return jax.shard_map(
        step,
        mesh=mesh,
        in_specs=(P("dp", None), P(None, "tp"), P(None, "tp"), P("tp", None)),
        out_specs=P("dp", None),
        check_vma=False,
    )
```

```python
import functools

import jax
import jax.numpy as jnp
from jax import lax
from jax.experimental import pallas as pl
from jax.experimental.pallas import tpu as pltpu
from jax.sharding import PartitionSpec as P

MESH = pl.DeviceIdType.MESH
FC = 256
YC = 512
NBUF = 8
W = 4
SHARED = 1
FIRST = 8
LAG_NB = 2
PIECES = 8
X0, Z0 = 6, 9
LAG_C, LAG_Z1, LAG_Z2, LAG_Z3 = 1, 4, 7, 9
B_PRIORITY = 1


def kernel(
    x_hbm, wg_hbm, wu_hbm, wd_hbm, y,
    xx, hidden, sent, ring, own, core_out, core_in, z_out, z_in1, z_in2,
    x_sem, ring_sem,
    core_ss, core_rs, z1_ss, z1_rs, z2_ss, z2_rs, z3_ss, z3_rs, fin_ss, fin_rs,
    xa_ss, xa_rs, xz_ss, xz_rs, xc_ss, xc_rs, xd_ss, xd_rs, h_ss, h_rs,
):
    rows, depth = x_hbm.shape
    half = rows // 2
    na = hidden.shape[0]
    nb = depth // YC
    ff = na * FC
    plain = na - 2 * SHARED
    first = min(FIRST, plain)
    loads = plain + SHARED
    quarter = depth // 4
    width = quarter // PIECES

    dp = lax.axis_index("dp")
    tp = lax.axis_index("tp")
    chip = tp // 2
    core = tp % 2
    side = dp // 2
    partner = (dp, tp + 1 - 2 * core)
    pair = (dp, tp + 2 - 4 * (chip % 2))
    cross = (dp, 2 * (3 - chip) + core)
    twin = ((dp + 2) % 4, tp)
    outer = (chip == 0) | (chip == 3)
    inner = jnp.logical_not(outer)
    mine = pl.ds(pl.multiple_of(core * half, half), half)
    theirs = pl.ds(pl.multiple_of((1 - core) * half, half), half)

    def chunk(i):
        shared = plain + 2 * (i - first) + side
        return jnp.where(i < first, i, jnp.where(i < first + SHARED, shared, i - SHARED))

    def load_a(w_hbm, i, which):
        slot = lax.rem(2 * i + which, NBUF)
        cols = pl.ds(pl.multiple_of(chunk(i) * FC, FC), FC)
        return pltpu.make_async_copy(w_hbm.at[:, cols], ring.at[slot], ring_sem.at[slot, 0])

    def load_b(j):
        slot = lax.rem(2 * loads + j, NBUF)
        return [
            pltpu.make_async_copy(
                wd_hbm.at[:, pl.ds(pl.multiple_of(j * YC + p * FC, FC), FC)],
                ring.at[slot, pl.ds(p * ff, ff)],
                ring_sem.at[slot, p],
            )
            for p in range(YC // FC)
        ]

    def start_b(j):
        for copy in load_b(j):
            copy.start(priority=B_PRIORITY)

    def start_item(i, which):
        @pl.when(i < loads)
        def _():
            load_a(wu_hbm if which else wg_hbm, i, which).start(priority=1)

        @pl.when((i >= loads) & (2 * (i - loads) + which < nb))
        def _():
            start_b(2 * (i - loads) + which)

    def remote(src, dst, ss, rs, c, to):
        return pltpu.make_async_remote_copy(
            src_ref=src, dst_ref=dst, send_sem=ss.at[c], recv_sem=rs.at[c],
            device_id=to, device_id_type=MESH,
        )

    def ycols(c):
        return pl.ds(pl.multiple_of(c * YC, YC), YC)

    def to_core(c):
        return remote(core_out.at[c], core_in.at[c], core_ss, core_rs, c, partner)

    def to_inner(c):
        return remote(z_out.at[c], z_in1.at[c], z1_ss, z1_rs, c, pair)

    def to_cross(c):
        return remote(z_out.at[c], z_in2.at[c], z2_ss, z2_rs, c, cross)

    def to_outer(c):
        part = y.at[mine, ycols(c)]
        return remote(part, part, z3_ss, z3_rs, c, pair)

    def to_partner(c):
        part = y.at[mine, ycols(c)]
        return remote(part, part, fin_ss, fin_rs, c, partner)

    def from_partner(c):
        part = y.at[theirs, ycols(c)]
        return remote(part, part, fin_ss, fin_rs, c, partner)

    def piece(z, c, k):
        return pl.ds(pl.multiple_of((2 * z + c) * quarter + k * width, width), width)

    zpar = chip % 2

    def x_to_twin(k):
        cols = piece(zpar, core, k)
        return remote(xx.at[0, :, cols], xx.at[1, :, cols], xa_ss, xa_rs, k, twin)

    def x_to_pair(k):
        part = xx.at[1, :, piece(zpar, core, k)]
        return remote(part, part, xz_ss, xz_rs, k, pair)

    def x_from_pair(k):
        part = xx.at[1, :, piece(1 - zpar, core, k)]
        return remote(part, part, xz_ss, xz_rs, k, pair)

    def x_to_core(k):
        part = xx.at[1, :, piece(zpar, core, k)]
        return remote(part, part, xc_ss, xc_rs, k, partner)

    def x_from_core(k):
        part = xx.at[1, :, piece(zpar, 1 - core, k)]
        return remote(part, part, xc_ss, xc_rs, k, partner)

    def xz_to_core(k):
        part = xx.at[1, :, piece(1 - zpar, core, k)]
        return remote(part, part, xd_ss, xd_rs, k, partner)

    def xz_from_core(k):
        part = xx.at[1, :, piece(1 - zpar, 1 - core, k)]
        return remote(part, part, xd_ss, xd_rs, k, partner)

    def h_to_twin(t):
        there = hidden.at[plain + 2 * t + side]
        return remote(sent.at[t], there, h_ss, h_rs, t, twin)

    def h_from_twin(t):
        here = hidden.at[plain + 2 * t + 1 - side]
        return remote(sent.at[t], here, h_ss, h_rs, t, twin)

    def forward(s):
        if not SHARED:
            return
        kx = s - X0

        @pl.when((kx >= 0) & (kx < PIECES))
        def _():
            x_to_twin(kx).wait_recv()
            x_to_pair(kx).start()
            x_to_core(kx).start()

        kz = s - Z0

        @pl.when((kz >= 0) & (kz < PIECES))
        def _():
            x_from_pair(kz).wait_recv()
            xz_to_core(kz).start()

    x_copies = [
        pltpu.make_async_copy(
            x_hbm.at[:, pl.ds(q * quarter, quarter)],
            xx.at[0, :, pl.ds(q * quarter, quarter)],
            x_sem.at[q],
        )
        for q in range(4)
    ]
    for copy in x_copies:
        copy.start()
    for n in range(W):
        load_a(wu_hbm if n % 2 else wg_hbm, n // 2, n % 2).start(priority=1)

    barrier = pltpu.get_barrier_semaphore()
    peers = [partner, pair] + ([twin] if SHARED else [])
    for peer in peers:
        pl.semaphore_signal(barrier, inc=1, device_id=peer, device_id_type=MESH)

    @pl.when(inner)
    def _():
        pl.semaphore_signal(barrier, inc=1, device_id=cross, device_id_type=MESH)

    for copy in x_copies:
        copy.wait()

    def meet():
        @pl.when(outer)
        def _():
            pl.semaphore_wait(barrier, len(peers))

        @pl.when(inner)
        def _():
            pl.semaphore_wait(barrier, len(peers) + 1)

    if SHARED:
        meet()
    if SHARED:
        for k in range(PIECES):
            x_to_twin(k).start()

    def gated(gate, up):
        return (jax.nn.silu(gate) * up).astype(jnp.bfloat16)

    def step_a(i, _):
        if SHARED:
            n = i - LAG_NB
            t = n - first

            @pl.when(t == 0)
            def _():
                def arrive(k, _):
                    x_from_core(k).wait_recv()
                    xz_from_core(k).wait_recv()
                    return 0

                lax.fori_loop(0, PIECES, arrive, 0)

            @pl.when((t >= 0) & (t < SHARED))
            def _():
                slot = lax.rem(2 * n, NBUF)
                gate = jnp.dot(xx[1], ring[slot], preferred_element_type=jnp.float32)
                up = jnp.dot(xx[1], ring[slot + 1], preferred_element_type=jnp.float32)
                sent[t] = gated(gate, up)
                h_to_twin(t).start()

        @pl.when(i < loads)
        def _():
            slot = lax.rem(2 * i, NBUF)
            forward(2 * i)
            load_a(wg_hbm, i, 0).wait()
            start_item(i + W // 2, W % 2)
            gate = jnp.dot(xx[0], ring[slot], preferred_element_type=jnp.float32)
            forward(2 * i + 1)
            load_a(wu_hbm, i, 1).wait()
            start_item(i + (W + 1) // 2, 1 - W % 2)
            up = jnp.dot(xx[0], ring[slot + 1], preferred_element_type=jnp.float32)
            hidden[chunk(i)] = gated(gate, up)

        return 0

    extra = max(0, first + SHARED + LAG_NB - loads) if SHARED else 0
    lax.fori_loop(0, loads + extra, step_a, 0)
    if not SHARED:
        meet()
    for t in range(SHARED):
        h_from_twin(t).wait_recv()

    def step_b(j, _):
        @pl.when(j < nb)
        def _():
            slot = lax.rem(2 * loads + j, NBUF)
            for copy in load_b(j):
                copy.wait()

            @pl.when(j + W < nb)
            def _():
                start_b(j + W)

            terms = [jnp.zeros((rows, FC), jnp.float32) for _ in range(YC // FC)]
            for k in range(na):
                for p in range(YC // FC):
                    at = p * ff + k * FC
                    terms[p] += jnp.dot(
                        hidden[k], ring[slot, at:at + FC, :],
                        preferred_element_type=jnp.float32,
                    )
            for p, term in enumerate(terms):
                cols = pl.ds(p * FC, FC)

                @pl.when(core == 0)
                def _():
                    own[j, :, cols] = term[:half]
                    core_out[j, :, cols] = term[half:].astype(jnp.bfloat16)

                @pl.when(core == 1)
                def _():
                    own[j, :, cols] = term[half:]
                    core_out[j, :, cols] = term[:half].astype(jnp.bfloat16)

            to_core(j).start()

        c1 = j - LAG_C

        @pl.when((c1 >= 0) & (c1 < nb))
        def _():
            to_core(c1).wait_recv()
            total = own[c1] + core_in[c1].astype(jnp.float32)

            @pl.when(outer)
            def _():
                z_out[c1] = total.astype(jnp.bfloat16)
                to_inner(c1).start()

            @pl.when(inner)
            def _():
                own[c1] = total

        c3 = j - LAG_Z2

        @pl.when(inner & (c3 >= 0) & (c3 < nb))
        def _():
            to_cross(c3).wait_recv()
            y[mine, ycols(c3)] = (
                z_out[c3].astype(jnp.float32) + z_in2[c3].astype(jnp.float32)
            ).astype(jnp.bfloat16)
            to_outer(c3).start()
            to_partner(c3).start()

        c2 = j - LAG_Z1

        @pl.when(inner & (c2 >= 0) & (c2 < nb))
        def _():
            to_inner(c2).wait_recv()
            z_out[c2] = (own[c2] + z_in1[c2].astype(jnp.float32)).astype(jnp.bfloat16)
            to_cross(c2).start()

        c4 = j - LAG_Z3

        @pl.when(outer & (c4 >= 0) & (c4 < nb))
        def _():
            to_outer(c4).wait_recv()
            to_partner(c4).start()

        return 0

    lax.fori_loop(0, nb + LAG_Z3, step_b, 0)

    def drain(c, _):
        to_core(c).wait_send()
        to_partner(c).wait_send()
        from_partner(c).wait_recv()

        @pl.when(outer)
        def _():
            to_inner(c).wait_send()

        @pl.when(inner)
        def _():
            to_cross(c).wait_send()
            to_outer(c).wait_send()

        return 0

    lax.fori_loop(0, nb, drain, 0)
    if SHARED:
        def drain_x(k, _):
            x_to_twin(k).wait_send()
            x_to_pair(k).wait_send()
            x_to_core(k).wait_send()
            xz_to_core(k).wait_send()
            return 0

        lax.fori_loop(0, PIECES, drain_x, 0)
        for t in range(SHARED):
            h_to_twin(t).wait_send()


def solution(mesh):
    def step(x, w_gate, w_up, w_down):
        rows, depth = x.shape
        ff = w_gate.shape[1]
        half = rows // 2
        na, nb = ff // FC, depth // YC
        bf16, f32 = jnp.bfloat16, jnp.float32
        hbm = pl.BlockSpec(memory_space=pltpu.HBM)
        dma = pltpu.SemaphoreType.DMA
        slots = max(SHARED, 1)
        return pl.pallas_call(
            kernel,
            out_shape=jax.ShapeDtypeStruct((rows, depth), bf16),
            in_specs=[hbm] * 4,
            out_specs=pl.BlockSpec(memory_space=pltpu.VMEM),
            scratch_shapes=[
                pltpu.VMEM((2, rows, depth), bf16),
                pltpu.VMEM((na, rows, FC), bf16),
                pltpu.VMEM((slots, rows, FC), bf16),
                pltpu.VMEM((NBUF, depth, FC), bf16),
                pltpu.VMEM((nb, half, YC), f32),
            ] + [pltpu.VMEM((nb, half, YC), bf16)] * 5 + [
                dma((4,)), dma((NBUF, 2)),
            ] + [dma((nb,))] * 10 + [dma((PIECES,))] * 8 + [dma((slots,))] * 2,
            compiler_params=pltpu.CompilerParams(
                collective_id=0, has_side_effects=True, vmem_limit_bytes=50 * 1024 * 1024
            ),
            cost_estimate=pl.CostEstimate(
                flops=6 * rows * depth * ff, bytes_accessed=6 * depth * ff, transcendentals=rows * ff
            ),
        )(pltpu.with_memory_space_constraint(x, pltpu.HBM), w_gate, w_up, w_down)

    return jax.shard_map(
        step,
        mesh=mesh,
        in_specs=(P("dp", None), P(None, "tp"), P(None, "tp"), P("tp", None)),
        out_specs=P("dp", None),
        check_vma=False,
    )
```
